128 devices in a mesh: grp: 2 (over core), head: 8 (over x, z_hi), seq: 8 (over z_lo, y).
Axes of the slice: x: 4, y: 4, z: 4 (z_hi: 2, z_lo: 2; z = z_hi * 2 + z_lo), core: 2. Of those that a mesh axis runs over, the one named last changes fastest.
Arguments:
- prompt: bfloat16 [12288, 8192], P(('grp', 'seq')), may hold values from -6 to 6
- gain: float32 [8192], replicated, may hold values from 0.5 to 6
- w_query: bfloat16 [8192, 8192], P(('grp', 'seq'), 'head'), may hold values from -0.0625 to 0.0625
- w_key: bfloat16 [8192, 1024], P(('grp', 'seq'), 'head'), may hold values from -0.0625 to 0.0625
- w_value: bfloat16 [8192, 1024], P(('grp', 'seq'), 'head'), may hold values from -0.0625 to 0.0625
- a_query: bfloat16 [256, 8192, 32], P('seq', 'head'), may hold values from -0.0625 to 0.0625
- b_query: bfloat16 [256, 32, 8192], P('seq', None, 'head'), may hold values from -1 to 1
- a_value: bfloat16 [256, 8192, 32], P('seq', 'head'), may hold values from -0.0625 to 0.0625
- b_value: bfloat16 [256, 32, 1024], P('seq', None, 'head'), may hold values from -1 to 1
- bounds: int32 [2, 257], replicated, may hold values from 0 to 6144, as said below
- decode_adapter: int32 [2, 64], P('grp', 'seq'), may hold values from 0 to 255, as said below
- decode_in: bfloat16 [4, 128, 8192], P(None, ('grp', 'seq')), may hold values from -6 to 6
Outputs:
- prefill_out: bfloat16 [12288, 8192], P(('grp', 'seq'), 'head')
- decode_out: bfloat16 [4, 128, 8192], P(None, ('grp', 'seq'), 'head')
The draws below stay inside these ranges and needn't reach their ends.
Inputs may be any that keep to these rules, and one draw needn't show every extreme that they name: `bounds`: row c holds where each adapter's segment of batch c begins, followed by 6144; it starts at 0 and never falls. Tokens k * 768 to (k + 1) * 768 - 1 are exactly the segments of adapters k * 32 to (k + 1) * 32 - 1, of which exactly 8 are nonempty; each nonempty segment is one prompt. `decode_adapter`: row j lists in rising order the adapters of the nonempty segments of batch 1 - j, one decode sequence for each prompt.
All inputs are finite; a program needn't handle non-finite values.
Results may differ from the reference program's by a relative error of at most 0.0085.
The reference program's roundings to bfloat16 on the way (of `normed`, `shrink` and `weights`) count: a program that leaves them out, or rounds other values in their place, can miss the bound.
Values may be sent and summed in bfloat16 or wider, within the bound.
No kernel may reach another device: no remote copies, remote signals or barrier semaphores. Data moves between devices by JAX's collectives and lax.ppermute only.
A program may use at most 192 MiB of HBM per device.

```python
import math
import jax
import jax.numpy as jnp
from jax import lax

D = 8192
HEADS = 64
KV = 8
HD = 128
RANK = 32
ADAPTERS = 256
TOK_DEV = 768
PROMPTS_DEV = 8
STEPS = 4
TOKENS = 6144
SEQS = 64
N_SEQ = 8


def block_layout(key):
    adp = ADAPTERS // N_SEQ
    pick_key, cut_key = jax.random.split(key)
    chosen = jnp.sort(jax.random.permutation(pick_key, adp)[:PROMPTS_DEV]).astype(jnp.int32)
    cuts = jnp.sort(jax.random.permutation(cut_key, TOK_DEV - 1)[:PROMPTS_DEV - 1] + 1).astype(jnp.int32)
    edges = jnp.concatenate([jnp.zeros((1,), jnp.int32), cuts, jnp.full((1,), TOK_DEV, jnp.int32)])
    lengths = edges[1:] - edges[:-1]
    counts = jnp.zeros((adp,), jnp.int32).at[chosen].set(lengths)
    return (counts, chosen)


def layout(key):
    adp = ADAPTERS // N_SEQ
    base = jax.random.fold_in(key, 9173)
    keys = jax.vmap(lambda number: jax.random.fold_in(base, number))(jnp.arange(2 * N_SEQ))
    counts, chosen = jax.vmap(block_layout)(keys)
    counts = counts.reshape(2, ADAPTERS)
    edges = jnp.concatenate([jnp.zeros((2, 1), jnp.int32), jnp.cumsum(counts, axis=1).astype(jnp.int32)], axis=1)
    offsets = (jnp.arange(N_SEQ, dtype=jnp.int32) * adp)[None, :, None]
    chosen = (chosen.reshape(2, N_SEQ, PROMPTS_DEV) + offsets).reshape(2, SEQS)
    return (edges, chosen)


def draw_bounds(key, part):
    return layout(key)[0]


def draw_decode_adapter(key, part):
    chosen = layout(key)[1]
    return jnp.stack([chosen[1], chosen[0]], axis=0)


def draw_gain(key, part):
    return jnp.exp(jax.random.uniform(key, (D,), jnp.float32, math.log(0.5), math.log(2.0)))


def block_scale(stream_key, extent, shards, low, top_value):
    def one(dim, blocks):
        steps = jax.random.uniform(jax.random.fold_in(jax.random.fold_in(stream_key, 6), dim), (blocks,), jnp.float32, low / len(shards), top_value / len(shards))
        return jnp.repeat(jnp.exp(steps), extent[dim] // blocks).reshape((-1,) + (1,) * (len(extent) - dim - 1))

    level = one(*shards[0])
    for cut in shards[1:]:
        level = level * one(*cut)
    return level


def normal_values(stream_key, dims, scale, limit, shards=(), kind=jnp.bfloat16):
    values = scale * jax.random.normal(stream_key, dims, jnp.float32)
    if shards:
        values = values * block_scale(stream_key, dims, shards, -0.22, 0.18)
    return jnp.clip(values, -limit, limit).astype(kind)


def setup_inputs(seed: int = 0) -> dict:
    splits = jax.random.split(jax.random.key(seed), 13)
    return {
        "prompt": normal_values(splits[0], (2 * TOKENS, D), 1.0, 6.0, ((0, 16),)),
        "gain": draw_gain(jax.random.fold_in(splits[12], 71), 0),
        "w_query": normal_values(splits[2], (D, HEADS * HD), D ** -0.5, 0.0625, ((0, 16), (1, 8))),
        "w_key": normal_values(splits[3], (D, KV * HD), D ** -0.5, 0.0625, ((0, 16), (1, 8))),
        "w_value": normal_values(splits[4], (D, KV * HD), D ** -0.5, 0.0625, ((0, 16), (1, 8))),
        "a_query": normal_values(splits[5], (ADAPTERS, D, RANK), D ** -0.5, 0.0625, ((0, 8), (1, 8))),
        "b_query": normal_values(splits[6], (ADAPTERS, RANK, HEADS * HD), RANK ** -0.5, 1.0, ((0, 8), (2, 8))),
        "a_value": normal_values(splits[7], (ADAPTERS, D, RANK), D ** -0.5, 0.0625, ((0, 8), (1, 8))),
        "b_value": normal_values(splits[8], (ADAPTERS, RANK, KV * HD), RANK ** -0.5, 1.0, ((0, 8), (2, 8))),
        "bounds": draw_bounds(jax.random.fold_in(splits[12], 71), 0),
        "decode_adapter": draw_decode_adapter(jax.random.fold_in(splits[12], 71), 0),
        "decode_in": normal_values(splits[11], (STEPS, 2 * SEQS, D), 1.0, 6.0, ((1, 16),)),
    }


THETA = 500000.0
EPS = 1e-05

def rows_norm(rows, gain):
    values = rows.astype(jnp.float32)
    power = lax.optimization_barrier(jnp.mean(values * values, axis=-1, keepdims=True))
    return (values * lax.rsqrt(power + EPS) * gain).astype(jnp.bfloat16)

def rotate(heads, position):
    half = heads.shape[-1] // 2
    freq = THETA ** (-jnp.arange(half, dtype=jnp.float32) / half)
    angle = position.astype(jnp.float32)[:, None, None] * freq
    cosine = jnp.cos(angle)
    sine = jnp.sin(angle)
    lower = heads[..., :half]
    upper = heads[..., half:]
    return jnp.concatenate([lower * cosine - upper * sine, upper * cosine + lower * sine], axis=-1)

def adapter_term(normed, onehot, a_block, b_block):
    count, width, rank = a_block.shape
    mixed = jnp.einsum('nd,adr->nar', normed.astype(jnp.float32), a_block.astype(jnp.float32))
    shrink = lax.optimization_barrier(jnp.sum(mixed * onehot[:, :, None], axis=1)).astype(jnp.bfloat16)
    spread = onehot.astype(jnp.bfloat16)[:, :, None] * shrink[:, None, :]
    spread = spread.reshape(normed.shape[0], count * rank)
    return jnp.dot(spread, b_block.reshape(count * rank, b_block.shape[2]), preferred_element_type=jnp.float32)

def prefill_attention(query, key, value, place, start):
    tok = query.shape[0]
    kv_heads = key.shape[1]
    query = query.reshape(tok, kv_heads, -1, key.shape[2])
    scores = jnp.einsum('qkgd,pkd->kgqp', query.astype(jnp.float32), key.astype(jnp.float32)) * HD ** (-0.5)
    allowed = (start[:, None] == start[None, :]) & (place[None, :] <= place[:, None])
    scores = jnp.where(allowed, scores, -1e+30)
    top = lax.optimization_barrier(jnp.max(scores, axis=-1, keepdims=True))
    expo = jnp.where(allowed, jnp.exp(scores - top), 0.0)
    total = lax.optimization_barrier(jnp.sum(expo, axis=-1))
    weights = expo.astype(jnp.bfloat16)
    mixed = jnp.einsum('kgqp,pkd->kgqd', weights.astype(jnp.float32), value.astype(jnp.float32)) / total[..., None]
    return jnp.transpose(mixed, (2, 0, 1, 3)).reshape(tok, -1).astype(jnp.bfloat16)

def decode_attention(query, key, value, cached_key, cached_value, seen):
    steps, seqs, kv_heads, head_dim = key.shape
    query = query.reshape(steps, seqs, kv_heads, -1, head_dim).astype(jnp.float32)
    old = jnp.einsum('tskgd,pkd->tskgp', query, cached_key.astype(jnp.float32)) * HD ** (-0.5)
    new = jnp.einsum('tskgd,uskd->tskgu', query, key.astype(jnp.float32)) * HD ** (-0.5)
    old_mask = jnp.broadcast_to(seen[None, :, None, None, :], old.shape)
    order = jnp.arange(steps, dtype=jnp.int32)
    causal = order[None, :] <= order[:, None]
    new_mask = jnp.broadcast_to(causal[:, None, None, None, :], new.shape)
    old = jnp.where(old_mask, old, -1e+30)
    new = jnp.where(new_mask, new, -1e+30)
    top = jnp.maximum(lax.optimization_barrier(jnp.max(old, axis=-1, keepdims=True)), lax.optimization_barrier(jnp.max(new, axis=-1, keepdims=True)))
    old_expo = jnp.where(old_mask, jnp.exp(old - top), 0.0)
    new_expo = jnp.where(new_mask, jnp.exp(new - top), 0.0)
    total = lax.optimization_barrier(jnp.sum(old_expo, axis=-1)) + lax.optimization_barrier(jnp.sum(new_expo, axis=-1))
    old_weights = old_expo.astype(jnp.bfloat16).astype(jnp.float32)
    new_weights = new_expo.astype(jnp.bfloat16).astype(jnp.float32)
    mixed = jnp.einsum('tskgp,pkd->tskgd', old_weights, cached_value.astype(jnp.float32))
    mixed = mixed + jnp.einsum('tskgu,uskd->tskgd', new_weights, value.astype(jnp.float32))
    mixed = mixed / total[..., None]
    return mixed.reshape(steps, seqs, -1).astype(jnp.bfloat16)

def reference(prompt, gain, w_query, w_key, w_value, a_query, b_query, a_value, b_value, bounds, decode_adapter, decode_in):
    adp = ADAPTERS // N_SEQ
    tokens = TOK_DEV * N_SEQ
    seqs = PROMPTS_DEV * N_SEQ
    prefill_parts = []
    decode_parts = [[], []]
    for batch in range(2):
        edges = bounds[batch]
        other = 1 - batch
        for block in range(N_SEQ):
            first = batch * tokens + block * TOK_DEV
            row = other * seqs + block * PROMPTS_DEV
            fresh = decode_in[:, row:row + PROMPTS_DEV].reshape(STEPS * PROMPTS_DEV, D)
            normed = rows_norm(jnp.concatenate([prompt[first:first + TOK_DEV], fresh], axis=0), gain)
            low = block * adp
            local = edges[low:low + adp + 1]
            place = block * TOK_DEV + jnp.arange(TOK_DEV, dtype=jnp.int32)
            hot_prompt = ((local[None, :-1] <= place[:, None]) & (place[:, None] < local[None, 1:])).astype(jnp.float32)
            chosen = decode_adapter[other, block * PROMPTS_DEV:(block + 1) * PROMPTS_DEV]
            numbers = low + jnp.arange(adp, dtype=jnp.int32)
            hot_seq = (chosen[:, None] == numbers[None, :]).astype(jnp.float32)
            onehot = jnp.concatenate([hot_prompt, jnp.tile(hot_seq, (STEPS, 1))], axis=0)
            start = lax.optimization_barrier(jnp.max(jnp.where(local[None, :-1] <= place[:, None], local[None, :-1], 0), axis=1))
            lower = edges[chosen]
            upper = edges[chosen + 1]
            step_pos = (upper - lower)[None, :] + jnp.arange(STEPS, dtype=jnp.int32)[:, None]
            position = jnp.concatenate([place - start, step_pos.reshape(-1)]).astype(jnp.int32)
            rows = normed.shape[0]
            query = jnp.dot(normed, w_query, preferred_element_type=jnp.float32)
            query = query + adapter_term(normed, onehot, a_query[low:low + adp], b_query[low:low + adp])
            key = jnp.dot(normed, w_key, preferred_element_type=jnp.float32)
            value = jnp.dot(normed, w_value, preferred_element_type=jnp.float32)
            value = value + adapter_term(normed, onehot, a_value[low:low + adp], b_value[low:low + adp])
            query = rotate(query.reshape(rows, HEADS, HD), position).astype(jnp.bfloat16)
            key = rotate(key.reshape(rows, KV, HD), position).astype(jnp.bfloat16)
            value = value.reshape(rows, KV, HD).astype(jnp.bfloat16)
            prefill_parts.append(prefill_attention(query[:TOK_DEV], key[:TOK_DEV], value[:TOK_DEV], place, start))
            seen = (lower[:, None] <= place[None, :]) & (place[None, :] < upper[:, None])
            decode_parts[other].append(decode_attention(query[TOK_DEV:].reshape(STEPS, PROMPTS_DEV, HEADS * HD), key[TOK_DEV:].reshape(STEPS, PROMPTS_DEV, KV, HD), value[TOK_DEV:].reshape(STEPS, PROMPTS_DEV, KV, HD), key[:TOK_DEV], value[:TOK_DEV], seen))
    prefill_out = jnp.concatenate(prefill_parts, axis=0)
    decode_out = jnp.concatenate(decode_parts[0] + decode_parts[1], axis=1)
    return (prefill_out, decode_out)
```

```python
import functools
import jax
import jax.numpy as jnp
from jax import lax
from jax.experimental import pallas as pl
from jax.experimental.pallas import tpu as pltpu
from jax.sharding import PartitionSpec as P


HD = 128
SLOTS = 8
RANK = 32
THETA = 500000.0
EPS = 1e-05
MIB = 1 << 20
F32 = jnp.float32
BF16 = jnp.bfloat16

ID_P, START_P, END_P, ID_D, LOW_D, HIGH_D, META = 0, 8, 16, 24, 32, 40, 64


def vmem(shape=None):
    return pl.BlockSpec(memory_space=pltpu.VMEM)


def anyspace():
    return pl.BlockSpec(memory_space=pl.ANY)


def smem():
    return pl.BlockSpec(memory_space=pltpu.SMEM)


def cost(flops, nbytes, trans=0):
    return pl.CostEstimate(flops=int(flops), bytes_accessed=int(nbytes), transcendentals=int(trans))


def along_y(x, d):
    return lax.ppermute(x, "seq", [(z * 4 + y, z * 4 + (y + d) % 4) for z in range(2) for y in range(4)])


def across_z(x):
    return lax.ppermute(x, "seq", [(i, i ^ 4) for i in range(8)])


def to_partner(x):
    return lax.ppermute(x, "grp", [(0, 1), (1, 0)])


def prep_kernel(tok, adp, bounds_ref, dec_ref, meta_ref):
    g = lax.axis_index("grp")
    blk = lax.axis_index("seq")
    low = blk * adp
    base = blk * tok

    def body(i, n):
        lo = bounds_ref[g, low + i]
        hi = bounds_ref[g, low + i + 1]
        m = jnp.minimum(n, SLOTS - 1)

        @pl.when(hi > lo)
        def _():
            meta_ref[ID_P + m] = i
            meta_ref[START_P + m] = lo - base
            meta_ref[END_P + m] = hi - base

        return n + (hi > lo).astype(jnp.int32)

    lax.fori_loop(0, adp, body, jnp.int32(0))
    for s in range(SLOTS):
        c = dec_ref[0, s]
        meta_ref[ID_D + s] = c - low
        meta_ref[LOW_D + s] = bounds_ref[1 - g, c] - base
        meta_ref[HIGH_D + s] = bounds_ref[1 - g, c + 1] - base


def prep(bounds, decode_adapter, tok, adp):
    return pl.pallas_call(
        functools.partial(prep_kernel, tok, adp),
        out_shape=jax.ShapeDtypeStruct((META,), jnp.int32),
        in_specs=[smem(), smem()],
        out_specs=smem(),
        name="prep",
    )(bounds, decode_adapter)


def norm_kernel(nblk, prompt_ref, fresh_ref, gain_ref, mine_ref, theirs_ref, feat_ref, buf):
    g = lax.axis_index("grp")
    head = lax.axis_index("head")
    half = mine_ref.shape[1]
    d_part = feat_ref.shape[1]

    def rows(ref):
        x = ref[...].astype(F32)
        power = jnp.mean(x * x, axis=-1, keepdims=True)
        buf[...] = (x * lax.rsqrt(power + EPS) * gain_ref[...]).astype(BF16)

    pl.when(pl.program_id(0) < nblk)(lambda: rows(prompt_ref))
    pl.when(pl.program_id(0) == nblk)(lambda: rows(fresh_ref))
    feat_ref[...] = buf[:, pl.ds(pl.multiple_of(head * d_part, d_part), d_part)]
    mine_ref[...] = buf[:, pl.ds(pl.multiple_of(g * half, half), half)]
    theirs_ref[...] = buf[:, pl.ds(pl.multiple_of((1 - g) * half, half), half)]


def norm(prompt, fresh, gain, d_part):
    tok, width = prompt.shape
    rb = fresh.shape[0]
    nblk = tok // rb
    total = tok + rb
    half = width // 2
    return pl.pallas_call(
        functools.partial(norm_kernel, nblk),
        grid=(nblk + 1,),
        out_shape=(
            jax.ShapeDtypeStruct((total, half), BF16),
            jax.ShapeDtypeStruct((total, half), BF16),
            jax.ShapeDtypeStruct((total, d_part), BF16),
        ),
        in_specs=[
            pl.BlockSpec((rb, width), lambda i: (jnp.minimum(i, nblk - 1), 0)),
            pl.BlockSpec((rb, width), lambda i: (0, 0)),
            pl.BlockSpec((1, width), lambda i: (0, 0)),
        ],
        out_specs=(
            pl.BlockSpec((rb, half), lambda i: (i, 0)),
            pl.BlockSpec((rb, half), lambda i: (i, 0)),
            pl.BlockSpec((rb, d_part), lambda i: (i, 0)),
        ),
        scratch_shapes=[pltpu.VMEM((rb, width), BF16)],
        compiler_params=pltpu.CompilerParams(dimension_semantics=("arbitrary",), vmem_limit_bytes=16 * MIB),
        cost_estimate=cost(8 * total * width, 4 * total * width),
        name="norm",
    )(prompt, fresh, gain)


def lane_table(meta_ref, base, width):
    group = lax.broadcasted_iota(jnp.int32, (1, width), 1) // RANK
    out = jnp.zeros((1, width), jnp.int32)
    for s in range(SLOTS):
        out = jnp.where(group == s, meta_ref[base + s], out)
    return out


def prompt_mask(meta_ref, tok):
    width = SLOTS * RANK
    row = lax.broadcasted_iota(jnp.int32, (tok, width), 0)
    return (row >= lane_table(meta_ref, START_P, width)) & (row < lane_table(meta_ref, END_P, width))


def decode_mask(nrow):
    width = SLOTS * RANK
    row = lax.broadcasted_iota(jnp.int32, (nrow, width), 0)
    lane = lax.broadcasted_iota(jnp.int32, (nrow, width), 1)
    return (row & (SLOTS - 1)) == lane // RANK


def shrink_kernel(tok, meta_ref, feat_ref, aq_ref, av_ref, out_ref, maps, sems):
    copies = []
    for t, ref in enumerate((aq_ref, av_ref)):
        for s in range(2 * SLOTS):
            at = ID_P + s if s < SLOTS else ID_D + s - SLOTS
            c = pltpu.make_async_copy(
                ref.at[meta_ref[at]], maps.at[t, pl.ds(s * RANK, RANK), :], sems.at[t, s]
            )
            c.start()
            copies.append(c)
    for c in copies:
        c.wait()
    total = feat_ref.shape[0]
    width = SLOTS * RANK
    half = total // 2
    hot = prompt_mask(meta_ref, tok)
    hot_d = decode_mask(total - tok)

    def fold(x):
        x = x[:, :128] + x[:, 128:]
        x = x + pltpu.roll(x, 64, 1)
        return x + pltpu.roll(x, 32, 1)

    dims = (((1,), (1,)), ((), ()))
    parts = []
    for t in range(2):
        p = lax.dot_general(feat_ref[:tok], maps[t, :width], dims, preferred_element_type=F32)
        d = lax.dot_general(feat_ref[tok:], maps[t, width:], dims, preferred_element_type=F32)
        p = fold(jnp.where(hot, p, 0.0))
        d = fold(jnp.where(hot_d, d, 0.0))
        parts.append(jnp.concatenate([p, d], axis=0))
    q, v = parts
    lane = lax.broadcasted_iota(jnp.int32, (half, 128), 1)
    lo = jnp.where(lane < 32, q[:half], v[:half])
    hi = jnp.where(lane < 96, q[half:], v[half:])
    out_ref[...] = jnp.where(lane < 64, lo, hi)


def shrink_partial(meta, feat, a_query, a_value, tok):
    total, d_part = feat.shape
    return pl.pallas_call(
        functools.partial(shrink_kernel, tok),
        out_shape=jax.ShapeDtypeStruct((total // 2, 128), F32),
        in_specs=[smem(), vmem(), anyspace(), anyspace()],
        out_specs=vmem(),
        scratch_shapes=[
            pltpu.VMEM((2, 2 * SLOTS * RANK, d_part), BF16),
            pltpu.SemaphoreType.DMA((2, 2 * SLOTS)),
        ],
        compiler_params=pltpu.CompilerParams(vmem_limit_bytes=24 * MIB),
        cost_estimate=cost(2 * total * d_part * 512, 4 * MIB),
        name="shrink",
    )(meta, feat, a_query, a_value)


def expand_kernel(tok, meta_ref, tot_ref, bq_hbm, bv_hbm, sq_ref, sv_ref, bq_ref, bv_ref, sems):
    copies = []
    for t, (src, dst) in enumerate(((bq_hbm, bq_ref), (bv_hbm, bv_ref))):
        for s in range(2 * SLOTS):
            at = ID_P + s if s < SLOTS else ID_D + s - SLOTS
            c = pltpu.make_async_copy(
                src.at[meta_ref[at]], dst.at[pl.ds(s * RANK, RANK), :], sems.at[t, s]
            )
            c.start()
            copies.append(c)
    half = tot_ref.shape[0]
    width = SLOTS * RANK
    lane = lax.broadcasted_iota(jnp.int32, (half, 128), 1)
    tot = tot_ref[...]
    hot = prompt_mask(meta_ref, tok)
    hot_d = decode_mask(2 * half - tok)

    def spread(j):
        y = jnp.where(lane // RANK == j, tot, 0.0)
        y = y + pltpu.roll(y, 64, 1)
        return y + pltpu.roll(y, 32, 1)

    for j, ref in ((0, sq_ref), (1, sv_ref)):
        x = jnp.concatenate([spread(j), spread(j + 2)], axis=0)
        x = jnp.concatenate([x, x], axis=1)
        ref[:tok, :width] = jnp.where(hot, x[:tok], 0.0).astype(BF16)
        ref[:tok, width:] = jnp.zeros((tok, width), BF16)
        ref[tok:, :width] = jnp.zeros((2 * half - tok, width), BF16)
        ref[tok:, width:] = jnp.where(hot_d, x[tok:], 0.0).astype(BF16)
    for c in copies:
        c.wait()


def expand(meta, tot, b_query, b_value, tok):
    total = 2 * tot.shape[0]
    width = 2 * SLOTS * RANK
    return pl.pallas_call(
        functools.partial(expand_kernel, tok),
        out_shape=(
            jax.ShapeDtypeStruct((total, width), BF16),
            jax.ShapeDtypeStruct((total, width), BF16),
            jax.ShapeDtypeStruct((width, b_query.shape[2]), BF16),
            jax.ShapeDtypeStruct((width, b_value.shape[2]), BF16),
        ),
        in_specs=[smem(), vmem(), anyspace(), anyspace()],
        out_specs=(vmem(),) * 4,
        scratch_shapes=[pltpu.SemaphoreType.DMA((2, 2 * SLOTS))],
        compiler_params=pltpu.CompilerParams(vmem_limit_bytes=16 * MIB),
        cost_estimate=cost(20 * total * width, 4 * MIB),
        name="expand",
    )(meta, tot, b_query, b_value)


def matmul_kernel(n, tile, first, *refs):
    offs_ref, mine_ref, recv_ref = refs[:3]
    w_refs = refs[3 : 3 + n]
    k = 3 + n + (0 if first else 2)
    acc_in = refs[3 + n : k]
    own_ref, oth_ref, xbuf, wbuf, sems = refs[k:]
    total = own_ref.shape[0]
    depth, cols = wbuf.shape[1:]

    def move(i):
        off = pl.multiple_of(offs_ref[i], depth)
        return (
            pltpu.make_async_copy(mine_ref.at[:, pl.ds(off, depth)], xbuf.at[i, pl.ds(0, total), :], sems.at[0, i]),
            pltpu.make_async_copy(recv_ref.at[:, pl.ds(off, depth)], xbuf.at[i, pl.ds(total, total), :], sems.at[1, i]),
        )

    for i in range(n):
        pltpu.make_async_copy(w_refs[i], wbuf.at[i], sems.at[2, i]).start()
        for c in move(i):
            c.start()

    def step(i, _):
        for c in move(i):
            c.wait()
        pltpu.make_async_copy(w_refs[0], wbuf.at[i], sems.at[2, i]).wait()
        for j in range(cols // tile):
            at = slice(j * tile, (j + 1) * tile)
            w = wbuf[i, :, at]
            for out, base, before in ((own_ref, 0, 0), (oth_ref, total, 1)):
                part = jnp.dot(xbuf[i, base : base + total], w, preferred_element_type=F32)
                if first:
                    so_far = jnp.where(i == 0, 0.0, out[:, at])
                else:
                    so_far = jnp.where(i == 0, acc_in[before][:, at], out[:, at])
                out[:, at] = so_far + part
        return 0

    lax.fori_loop(0, n, step, 0)


def matmul(name, offs, mine, recv, pieces, before=None):
    n = len(pieces)
    total = mine.shape[0]
    depth, cols = pieces[0].shape
    first = before is None
    tile = 256 if cols % 256 == 0 else 128
    out = jax.ShapeDtypeStruct((total, cols), F32)
    return pl.pallas_call(
        functools.partial(matmul_kernel, n, tile, first),
        out_shape=(out, out),
        in_specs=[smem()] + [anyspace()] * (2 + n) + ([] if first else [vmem()] * 2),
        out_specs=(vmem(), vmem()),
        scratch_shapes=[
            pltpu.VMEM((n, 2 * total, depth), BF16),
            pltpu.VMEM((n, depth, cols), BF16),
            pltpu.SemaphoreType.DMA((3, n)),
        ],
        compiler_params=pltpu.CompilerParams(vmem_limit_bytes=44 * MIB),
        cost_estimate=cost(4 * n * depth * total * cols, n * depth * (4 * total + 2 * cols) + 8 * total * cols),
        name=name,
    )(offs, mine, recv, *pieces, *(() if first else before))


def rotated(x, cos_ref, sin_ref):
    return x * cos_ref[...] + pltpu.roll(x, HD // 2, 1) * sin_ref[...]


def kv_kernel(own_ref, recv_ref, sv_ref, bv_ref, cos_ref, sin_ref, kvp_ref, kvd_ref):
    tok = kvp_ref.shape[0]
    key = own_ref[:, :HD] + recv_ref[:, :HD]
    key = rotated(key, cos_ref, sin_ref).astype(BF16)
    value = own_ref[:, HD:] + recv_ref[:, HD:]
    value = (value + jnp.dot(sv_ref[...], bv_ref[...], preferred_element_type=F32)).astype(BF16)
    kvp_ref[:, :HD] = key[:tok]
    kvd_ref[:, :HD] = key[tok:]
    kvp_ref[:, HD:] = value[:tok]
    kvd_ref[:, HD:] = value[tok:]


def make_kv(own, recv, sv, bv, cos, sin, tok):
    total = sv.shape[0]
    whole = lambda shape: pl.BlockSpec(shape, lambda i: (0, 0))
    return pl.pallas_call(
        kv_kernel,
        grid=(1,),
        out_shape=(
            jax.ShapeDtypeStruct((tok, 2 * HD), BF16),
            jax.ShapeDtypeStruct((total - tok, 2 * HD), BF16),
        ),
        in_specs=[
            whole((total, 2 * HD)),
            whole((total, 2 * HD)),
            whole(sv.shape),
            whole(bv.shape),
            whole(cos.shape),
            whole(sin.shape),
        ],
        out_specs=(whole((tok, 2 * HD)), whole((total - tok, 2 * HD))),
        compiler_params=pltpu.CompilerParams(vmem_limit_bytes=24 * MIB),
        cost_estimate=cost(2 * total * 512 * HD, 4 * MIB),
        name="keyvalue",
    )(own, recv, sv, bv, cos, sin)


TILE = 256


def attend_kernel(aliased, *refs):
    meta_ref, own_ref, recv_ref, sq_ref, bq_ref, cos_ref, sin_ref, kv_ref = refs[:8]
    out_ref, dec_ref, qbuf, bias = refs[8 + aliased :]
    tok = out_ref.shape[0]

    @pl.when(pl.program_id(0) == 0)
    def _():
        for i in range(tok // TILE):
            row = lax.broadcasted_iota(jnp.int32, (TILE, 1), 0) + i * TILE
            start = jnp.zeros((TILE, 1), jnp.int32)
            for s in range(SLOTS):
                at = meta_ref[START_P + s]
                start = jnp.where(row >= at, at, start)
            n = (i + 1) * TILE
            col = lax.broadcasted_iota(jnp.int32, (TILE, n), 1)
            bias[i * TILE : (i + 1) * TILE, :n] = jnp.where((col >= start) & (col <= row), 0.0, -1e30)

    q = own_ref[...] + recv_ref[...]
    q = q + jnp.dot(sq_ref[...], bq_ref[...], preferred_element_type=F32)
    q = rotated(q, cos_ref, sin_ref).astype(BF16)
    dec_ref[...] = q[tok:]
    qbuf[...] = q[:tok]
    for i in range(tok // TILE):
        n = (i + 1) * TILE
        rows = slice(i * TILE, n)
        s = lax.dot_general(
            qbuf[rows], kv_ref[:n, :HD], (((1,), (1,)), ((), ())), preferred_element_type=F32
        )
        s = s * HD ** (-0.5) + bias[rows, :n]
        top = jnp.max(s, axis=-1, keepdims=True)
        e = jnp.exp(s - top)
        total = jnp.sum(e, axis=-1, keepdims=True)
        mixed = jnp.dot(e.astype(BF16), kv_ref[:n, HD:], preferred_element_type=F32)
        out_ref[rows] = (mixed / total).astype(BF16)


def attend(name, meta, own, recv, sq, bq, cos, sin, kvp, first_col, first_head, heads, cols, so_far=None):
    total = own.shape[0]
    tok = kvp.shape[0]
    whole = lambda shape: pl.BlockSpec(shape, lambda h: (0, 0))
    args = [meta, own, recv, sq, bq, cos, sin, kvp]
    specs = [
        smem(),
        pl.BlockSpec((total, HD), lambda h: (0, h + first_col)),
        pl.BlockSpec((total, HD), lambda h: (0, h + first_col)),
        whole(sq.shape),
        pl.BlockSpec((sq.shape[1], HD), lambda h: (0, h + first_head)),
        whole(cos.shape),
        whole(sin.shape),
        whole(kvp.shape),
    ]
    aliases = {}
    if so_far is not None:
        args.append(so_far)
        specs.append(anyspace())
        aliases = {8: 0}
    return pl.pallas_call(
        functools.partial(attend_kernel, len(aliases)),
        grid=(heads,),
        out_shape=(
            jax.ShapeDtypeStruct((tok, cols), BF16),
            jax.ShapeDtypeStruct((total - tok, heads * HD), BF16),
        ),
        in_specs=specs,
        out_specs=(
            pl.BlockSpec((tok, HD), lambda h: (0, h + first_head)),
            pl.BlockSpec((total - tok, HD), lambda h: (0, h)),
        ),
        scratch_shapes=[pltpu.VMEM((tok, HD), BF16), pltpu.VMEM((tok, tok), F32)],
        input_output_aliases=aliases,
        compiler_params=pltpu.CompilerParams(dimension_semantics=("arbitrary",), vmem_limit_bytes=32 * MIB),
        cost_estimate=cost(heads * 2 * (total * 512 * HD + 2 * tok * tok * HD), 4 * MIB, heads * tok * tok),
        name=name,
    )(*args)


def decode_kernel(nq, meta_ref, *refs):
    q_refs = refs[:nq]
    kvd_ref, cached_ref, out_ref = refs[nq:]
    tok = cached_ref.shape[0]
    nrow = kvd_ref.shape[0]
    heads = [(r, h) for r in q_refs for h in range(r.shape[1] // HD)]
    q = jnp.concatenate([r[:, h * HD : (h + 1) * HD] for r, h in heads], axis=0)
    m = q.shape[0]
    seq = lax.broadcasted_iota(jnp.int32, (m, 1), 0)
    step = (seq & (nrow - 1)) // SLOTS
    seq = seq & (SLOTS - 1)
    lower = jnp.zeros((m, 1), jnp.int32)
    upper = jnp.zeros((m, 1), jnp.int32)
    for s in range(SLOTS):
        lower = jnp.where(seq == s, meta_ref[LOW_D + s], lower)
        upper = jnp.where(seq == s, meta_ref[HIGH_D + s], upper)
    dims = (((1,), (1,)), ((), ()))
    old = lax.dot_general(q, cached_ref[:, :HD], dims, preferred_element_type=F32) * HD ** (-0.5)
    new = lax.dot_general(q, kvd_ref[:, :HD], dims, preferred_element_type=F32) * HD ** (-0.5)
    col = lax.broadcasted_iota(jnp.int32, (m, tok), 1)
    old = jnp.where((col >= lower) & (col < upper), old, -1e30)
    col = lax.broadcasted_iota(jnp.int32, (m, nrow), 1)
    new = jnp.where(((col & (SLOTS - 1)) == seq) & (col // SLOTS <= step), new, -1e30)
    top = jnp.maximum(jnp.max(old, axis=-1, keepdims=True), jnp.max(new, axis=-1, keepdims=True))
    old = jnp.exp(old - top)
    new = jnp.exp(new - top)
    total = jnp.sum(old, axis=-1, keepdims=True) + jnp.sum(new, axis=-1, keepdims=True)
    mixed = jnp.dot(old.astype(BF16), cached_ref[:, HD:], preferred_element_type=F32)
    mixed = mixed + jnp.dot(new.astype(BF16), kvd_ref[:, HD:], preferred_element_type=F32)
    mixed = (mixed / total).astype(BF16)
    for i in range(len(heads)):
        out_ref[:, i * HD : (i + 1) * HD] = mixed[i * nrow : (i + 1) * nrow]


def decode(meta, queries, kvd, cached):
    cols = sum(q.shape[1] for q in queries)
    return pl.pallas_call(
        functools.partial(decode_kernel, len(queries)),
        out_shape=jax.ShapeDtypeStruct((kvd.shape[0], cols), BF16),
        in_specs=[smem()] + [vmem()] * (len(queries) + 2),
        out_specs=vmem(),
        compiler_params=pltpu.CompilerParams(vmem_limit_bytes=16 * MIB),
        cost_estimate=cost(4 * 256 * 800 * HD, MIB, 256 * 800),
        name="decode",
    )(meta, *queries, kvd, cached)


def gather(own, kind):
    a = along_y(own, 1)
    b = along_y(own, -1)
    zp = across_z(own)
    if kind == "y":
        za = along_y(zp, 1)
        zb = along_y(zp, -1)
        e = along_y(a, 1)
        ze = along_y(zb, -1)
    else:
        e = along_y(b, -1)
        za = across_z(a)
        zb = across_z(b)
        ze = across_z(e)
    return own, zp, a, b, e, za, zb, ze


def per_device(
    prompt, gain, w_query, w_key, w_value, a_query, b_query, a_value, b_value, bounds, decode_adapter, decode_in
):
    tok, width = prompt.shape
    steps, seqs, _ = decode_in.shape
    fresh = decode_in.reshape(steps * seqs, width)
    adp, d_part, rank = a_query.shape
    q_cols = w_query.shape[1]
    depth = w_query.shape[0]
    blk = lax.axis_index("seq")

    c0 = jnp.concatenate([w_key, w_value, w_query[:, :384]], axis=1)
    c1 = w_query[:, 384:768]
    c2 = w_query[:, 768:]
    g1 = gather(c1, "z")
    g0 = gather(c0, "y")
    g2 = gather(c2, "z")
    y = blk % 4
    z = blk - y
    oz = 4 - z
    ring = lambda base, d: base + (y + d) % 4
    where = jnp.stack([blk, oz + y, ring(z, 3), ring(z, 1), ring(z, 2), ring(oz, 3), ring(oz, 1), ring(oz, 2)])
    offs = (where * depth).astype(jnp.int32)

    meta = prep(bounds, decode_adapter, tok, adp)
    mine, theirs, feat = norm(prompt, fresh, gain.reshape(1, width), d_part)
    recv = to_partner(theirs)

    part = shrink_partial(meta, feat, jnp.swapaxes(a_query, 1, 2), jnp.swapaxes(a_value, 1, 2), tok)
    for pairs in ([i ^ 1 for i in range(8)], [i ^ 2 for i in range(8)], [i ^ 6 for i in range(8)]):
        part = part + lax.ppermute(part, "head", list(enumerate(pairs)))
    sq, sv, bq, bv = expand(meta, part, b_query, b_value, tok)

    row = jnp.arange(tok, dtype=jnp.int32)
    starts = meta[START_P : START_P + SLOTS]
    start = jnp.max(jnp.where(starts[None, :] <= row[:, None], starts[None, :], 0), axis=1)
    lengths = meta[HIGH_D : HIGH_D + SLOTS] - meta[LOW_D : LOW_D + SLOTS]
    step_pos = lengths[None, :] + jnp.arange(steps, dtype=jnp.int32)[:, None]
    position = jnp.concatenate([row - start, step_pos.reshape(-1)])
    half = HD // 2
    freq = THETA ** (-jnp.arange(half, dtype=F32) / half)
    angle = position.astype(F32)[:, None] * freq
    cosine = jnp.cos(angle)
    sine = jnp.sin(angle)
    cos = jnp.concatenate([cosine, cosine], axis=1)
    sin = jnp.concatenate([-sine, sine], axis=1)

    order = (0, 1, 2, 3)
    late = (4, 5, 6, 7)
    m0 = matmul("m0a", offs[:4], mine, recv, [g0[i] for i in order])
    own0, oth0 = matmul("m0b", offs[4:], mine, recv, [g0[i] for i in late], m0)
    got0 = to_partner(oth0)
    own1, oth1 = matmul("m1", offs, mine, recv, g1)
    got1 = to_partner(oth1)
    kvp, kvd = make_kv(own0, got0, sv, bv, cos, sin, tok)
    cached = to_partner(kvp)
    out, qd0 = attend("f0", meta, own0, got0, sq, bq, cos, sin, kvp, 2, 0, 3, q_cols)
    out, qd1 = attend("f1", meta, own1, got1, sq, bq, cos, sin, kvp, 0, 3, 3, q_cols, out)
    own2, oth2 = matmul("m2", offs, mine, recv, g2)
    got2 = to_partner(oth2)
    out, qd2 = attend("f2", meta, own2, got2, sq, bq, cos, sin, kvp, 0, 6, 2, q_cols, out)
    dec = decode(meta, (qd0, qd1, qd2), kvd, cached)
    return out, dec.reshape(steps, seqs, q_cols)


def solution(mesh):
    placed = (
        P(("grp", "seq"), None),
        P(),
        P(("grp", "seq"), "head"),
        P(("grp", "seq"), "head"),
        P(("grp", "seq"), "head"),
        P("seq", "head", None),
        P("seq", None, "head"),
        P("seq", "head", None),
        P("seq", None, "head"),
        P(),
        P("grp", "seq"),
        P(None, ("grp", "seq"), None),
    )
    return jax.shard_map(
        per_device,
        mesh=mesh,
        in_specs=placed,
        out_specs=(P(("grp", "seq"), "head"), P(None, ("grp", "seq"), "head")),
        check_vma=False,
    )
```
